256 devices in a mesh: gx: 32 (over z, y), gy: 4 (over x_lo, core), gz: 2 (over x_hi).
Axes of the slice: x: 4 (x_hi: 2, x_lo: 2; x = x_hi * 2 + x_lo), y: 4, z: 8, core: 2. Of those that a mesh axis runs over, the one named last changes fastest.
Arguments:
- weights: float32 [3, 128, 128, 512], P(None, 'gx', 'gz', 'gy'), may hold values from 0.2 to 2
- abscissas: float32 [3, 128, 128, 512], P(None, 'gx', 'gz', 'gy'), may hold values from -4 to 4, as said below
Outputs:
- moments_end: float32 [6, 128, 128, 512], P(None, 'gx', 'gz', 'gy')
The draws below stay inside these ranges and needn't reach their ends.
Inputs may be any that keep to these rules, and one draw needn't show every extreme that they name: In every cell the three abscissas increase with the node index, consecutive ones at least 0.25 apart.
All inputs are finite; a program needn't handle non-finite values. Where the reference program divides by a largest or mean magnitude, that divisor is 1e-20 or more.
Results may differ from the reference program's by a relative error of at most 0.0003.
Values sent between devices are 32-bit elements; how exact they have to be, the bound alone decides.
No kernel may reach another device: no remote copies, remote signals or barrier semaphores. Data moves between devices by JAX's collectives and lax.ppermute only.
A program may use at most 128 MiB of HBM per device.

```python
import math
import jax
import jax.numpy as jnp
from jax import lax

NODES = 3
NX = 128
NZ = 128
NY = 512


def draw_abscissas(key, part):
    noise_key = jax.random.fold_in(key, 11)
    place_key = jax.random.fold_in(key, 23)
    height_key = jax.random.fold_in(key, 37)
    noise = jax.random.uniform(noise_key, (NODES, NX, NZ, NY), jnp.float32, -0.25, 0.25)
    centres = jnp.array([-1.0, 0.0, 1.0], jnp.float32).reshape(3, 1, 1, 1)
    position = (jnp.arange(NX, dtype=jnp.float32) + 0.5) / NX
    window_start = jax.random.randint(place_key, (), 0, NX - 3)
    height = jax.random.uniform(height_key, (), jnp.float32, 1.6, 3.2)
    cell_index = jnp.arange(NX, dtype=jnp.int32)
    inside = (cell_index >= window_start) & (cell_index < window_start + 4)
    factor = jnp.where(inside, height, 0.5 + position).reshape(1, NX, 1, 1)
    return ((centres + noise) * factor).astype(jnp.float32)


def block_scale(stream_key, dims, cuts, least, largest):
    gain = 1.0
    for dim, shards_of in cuts:
        heights = jax.random.uniform(jax.random.fold_in(jax.random.fold_in(stream_key, 6), dim), (shards_of,), jnp.float32, least / len(cuts), largest / len(cuts))
        gain = gain * jnp.repeat(jnp.exp(heights), dims[dim] // shards_of).reshape((-1,) + (1,) * (len(dims) - 1 - dim))
    return gain


def setup_inputs(seed: int = 0) -> dict:
    streams_of = jax.random.split(jax.random.key(seed), 3)
    return {
        "weights": jnp.clip(jnp.exp(math.log(2.0) - 2.3025851 * jax.random.uniform(streams_of[0], (NODES, NX, NZ, NY), jnp.float32) ** block_scale(streams_of[0], (NODES, NX, NZ, NY), ((1, 32), (2, 2), (3, 4)), -0.2, 0.2)), 0.2, 2.0),
        "abscissas": draw_abscissas(jax.random.fold_in(streams_of[2], 71), 0),
    }


COURANT = 0.4
SPEED_TOTAL = 1.72
AXIS_SPEEDS = ((1, 0.6), (2, 0.64), (3, 0.48))

def minmod(first, second):
    return jnp.where(first * second > 0.0, jnp.sign(first) * jnp.minimum(jnp.abs(first), jnp.abs(second)), 0.0)

def cut_along(array, lower, upper, array_axis):
    return lax.slice_in_dim(array, lower, upper, axis=array_axis)

def moments_of(node_weights, node_speeds):
    result = []
    power = node_weights
    for order in range(6):
        result.append(lax.optimization_barrier(jnp.sum(power, axis=0)))
        power = power * node_speeds
    return jnp.stack(result)

def face_divergence(node_weights, node_speeds):
    total = None
    for array_axis, component in AXIS_SPEEDS:
        window = [slice(None), slice(2, -2), slice(2, -2), slice(2, -2)]
        window[array_axis] = slice(None)
        line_w = node_weights[tuple(window)]
        line_u = node_speeds[tuple(window)]
        length = line_w.shape[array_axis]
        jumps = cut_along(line_w, 1, length, array_axis) - cut_along(line_w, 0, length - 1, array_axis)
        slopes = minmod(cut_along(jumps, 0, length - 2, array_axis), cut_along(jumps, 1, length - 1, array_axis))
        left_w = cut_along(line_w, 1, length - 2, array_axis) + 0.5 * cut_along(slopes, 0, length - 3, array_axis)
        right_w = cut_along(line_w, 2, length - 1, array_axis) - 0.5 * cut_along(slopes, 1, length - 2, array_axis)
        left_u = cut_along(line_u, 1, length - 2, array_axis)
        right_u = cut_along(line_u, 2, length - 1, array_axis)
        left_term = component * left_w * jnp.maximum(left_u, 0.0)
        right_term = component * right_w * jnp.minimum(right_u, 0.0)
        fluxes = []
        for order in range(6):
            fluxes.append(lax.optimization_barrier(jnp.sum(left_term + right_term, axis=0)))
            left_term = left_term * left_u
            right_term = right_term * right_u
        flux = jnp.stack(fluxes)
        faces = length - 3
        diverge = cut_along(flux, 1, faces, array_axis) - cut_along(flux, 0, faces - 1, array_axis)
        total = diverge if total is None else total + diverge
    return total

def invert(moments):
    mom = [moments[index] for index in range(6)]
    mean_one = mom[1] / mom[0]
    first_row = [None] + [mom[level + 1] - mean_one * mom[level] for level in range(1, 5)]
    mean_two = first_row[2] / first_row[1] - mean_one
    spread_one = first_row[1] / mom[0]
    second_two = first_row[3] - mean_two * first_row[2] - spread_one * mom[2]
    second_three = first_row[4] - mean_two * first_row[3] - spread_one * mom[3]
    mean_three = second_three / second_two - first_row[2] / first_row[1]
    spread_two = second_two / first_row[1]
    centre = (mean_one + mean_two + mean_three) / 3.0
    dev_one = mean_one - centre
    dev_two = mean_two - centre
    dev_three = mean_three - centre
    radius = jnp.sqrt((dev_one * dev_one + dev_two * dev_two + dev_three * dev_three + 2.0 * spread_one + 2.0 * spread_two) / 6.0)
    determinant = dev_one * dev_two * dev_three - dev_one * spread_two - dev_three * spread_one
    ratio = determinant / (2.0 * radius * radius * radius)
    angle = jnp.arccos(ratio) / 3.0
    highest = centre + 2.0 * radius * jnp.cos(angle)
    lowest = centre + 2.0 * radius * jnp.cos(angle + 2.0 * math.pi / 3.0)
    middle = 3.0 * centre - highest - lowest
    root_one = jnp.sqrt(spread_one)
    root_two = jnp.sqrt(spread_two)
    speeds = []
    masses = []
    for value in (lowest, middle, highest):
        first_comp = (value - mean_one) / root_one
        second_comp = ((value - mean_two) * first_comp - root_one) / root_two
        masses.append(mom[0] / (1.0 + first_comp * first_comp + second_comp * second_comp))
        speeds.append(value)
    return (jnp.stack(masses), jnp.stack(speeds))

def periodic(array):
    return jnp.pad(array, ((0, 0), (2, 2), (2, 2), (2, 2)), mode='wrap')

def reference(weights, abscissas):
    moments_start = moments_of(weights, abscissas)
    step_one = COURANT / (SPEED_TOTAL * jnp.max(jnp.abs(abscissas)))
    moments_mid = moments_start - step_one * face_divergence(periodic(weights), periodic(abscissas))
    mid_weights, mid_speeds = invert(moments_mid)
    step_two = COURANT / (SPEED_TOTAL * jnp.max(jnp.abs(mid_speeds)))
    change = face_divergence(periodic(mid_weights), periodic(mid_speeds))
    return 0.5 * moments_start + 0.5 * (moments_mid - step_two * change)
```

```python
import math

import numpy as np
import jax
import jax.numpy as jnp
from jax import lax
from jax.experimental import pallas as pl
from jax.experimental.pallas import tpu as pltpu
from jax.sharding import PartitionSpec as P

AXES = ("gx", "gy", "gz")
COURANT = 0.4
SPEED_TOTAL = 1.72
SPEED_X, SPEED_Z, SPEED_Y = 0.6, 0.64, 0.48
ROWS = 8


def root_table(degree):
    points = np.cos((np.arange(400) + 0.5) * np.pi / 400)
    values = np.cos(2.0 / 3.0 * np.arccos(0.5 * (points + 1.0)))
    fit = np.polynomial.chebyshev.Chebyshev.fit(points, values, degree, domain=[-1, 1])
    return [float(c) for c in fit.convert(kind=np.polynomial.Polynomial).coef]


ROOT = root_table(11)


def cos_third(ratio):
    half = jnp.sqrt(jnp.maximum(0.5 + 0.5 * ratio, 0.0))
    t = 2.0 * half - 1.0
    total = jnp.full_like(t, ROOT[-1])
    for c in ROOT[-2::-1]:
        total = total * t + c
    return total


def limited(a, b):
    return jnp.maximum(jnp.minimum(a, b), 0.0) + jnp.minimum(jnp.maximum(a, b), 0.0)


def side_terms(c, wm2, wm1, w, wp1, wp2, um1, u, up1):
    d0, d1, d2, d3 = wm1 - wm2, w - wm1, wp1 - w, wp2 - wp1
    below = limited(d0, d1)
    here = (0.5 * c) * limited(d1, d2)
    above = limited(d2, d3)
    base = c * w
    own = (base + here) * jnp.maximum(u, 0.0) - (base - here) * jnp.minimum(u, 0.0)
    low = (wm1 + 0.5 * below) * (c * jnp.minimum(-um1, 0.0))
    high = (wp1 - 0.5 * above) * (c * jnp.minimum(up1, 0.0))
    return own, low, high


class Fields:
    def __init__(self, w, u, pw, pu, xlo, xhi, ylo, yhi):
        self.w, self.u, self.pw, self.pu = w, u, pw, pu
        self.xlo, self.xhi, self.ylo, self.yhi = xlo, xhi, ylo, yhi

    def plane_w(self, n, x, z):
        if x == -1:
            return self.xlo[n, z, :]
        if x == -2:
            return self.xlo[6 + n, z, :]
        if x == 4:
            return self.xhi[n, z, :]
        if x == 5:
            return self.xhi[6 + n, z, :]
        return self.w[n, x, z, :]

    def plane_u(self, n, x, z):
        if x == -1:
            return self.xlo[3 + n, z, :]
        if x == 4:
            return self.xhi[3 + n, z, :]
        return self.u[n, x, z, :]


def pad_rows(f, zr):
    def copy(i, carry):
        z = pl.ds(pl.multiple_of(i * ROWS, ROWS), ROWS)
        zp = pl.ds(pl.multiple_of(i * ROWS + 8, ROWS), ROWS)
        f.pw[:, :, zp, :] = f.w[:, :, z, :]
        f.pu[:, :, zp, :] = f.u[:, :, z, :]
        return carry

    lax.fori_loop(0, 64 // ROWS, copy, 0)
    f.pw[:, :, 7, :] = zr[0, 0:3]
    f.pu[:, :, 7, :] = zr[0, 3:6]
    f.pw[:, :, 6, :] = zr[0, 6:9]
    f.pw[:, :, 72, :] = zr[1, 0:3]
    f.pu[:, :, 72, :] = zr[1, 3:6]
    f.pw[:, :, 73, :] = zr[1, 6:9]


def divergence(f, i, x, lane):
    z0 = i * ROWS
    z = pl.ds(pl.multiple_of(z0, ROWS), ROWS)
    first, final = lane == 0, lane == 127
    hlo, hhi = f.ylo[z, :], f.yhi[z, :]

    def halo_lo(k):
        return pltpu.roll(hlo, (128 - (4 * k + x)) % 128, 1)

    def halo_hi(k):
        return pltpu.roll(hhi, 127 - (4 * k + x), 1)

    total = [None] * 6
    nodes = []
    for n in range(3):
        w, u = f.w[n, x, z, :], f.u[n, x, z, :]
        nodes.append((w, u))
        parts = []
        um1, up1 = f.plane_u(n, x - 1, z), f.plane_u(n, x + 1, z)
        own, low, high = side_terms(
            SPEED_X, *[f.plane_w(n, x + s, z) for s in (-2, -1)], w,
            *[f.plane_w(n, x + s, z) for s in (1, 2)], um1, u, up1)
        parts += [(low, um1), (high, up1)]

        def row_w(s):
            return f.pw[n, x, pl.ds(z0 + 8 + s, ROWS), :]

        um1, up1 = f.pu[n, x, pl.ds(z0 + 7, ROWS), :], f.pu[n, x, pl.ds(z0 + 9, ROWS), :]
        own_z, low, high = side_terms(
            SPEED_Z, row_w(-2), row_w(-1), w, row_w(1), row_w(2), um1, u, up1)
        parts += [(low, um1), (high, up1)]
        own = own + own_z
        um1 = jnp.where(first, halo_lo(3 + n), pltpu.roll(u, 1, 1))
        up1 = jnp.where(final, halo_hi(3 + n), pltpu.roll(u, 127, 1))
        wm1 = jnp.where(first, halo_lo(n), pltpu.roll(w, 1, 1))
        wp1 = jnp.where(final, halo_hi(n), pltpu.roll(w, 127, 1))
        wm2 = jnp.where(first, halo_lo(6 + n), pltpu.roll(wm1, 1, 1))
        wp2 = jnp.where(final, halo_hi(6 + n), pltpu.roll(wp1, 127, 1))
        own_y, low, high = side_terms(SPEED_Y, wm2, wm1, w, wp1, wp2, um1, u, up1)
        parts += [(low, um1), (high, up1)]
        own = own + own_y
        parts.append((own, u))
        for order in range(6):
            term = parts[0][0]
            for value, _ in parts[1:]:
                term = term + value
            total[order] = term if total[order] is None else total[order] + term
            if order < 5:
                parts = [(value * speed, speed) for value, speed in parts]
    return total, nodes


def moments_of(nodes):
    total = [None] * 6
    for w, u in nodes:
        power = w
        for order in range(6):
            total[order] = power if total[order] is None else total[order] + power
            if order < 5:
                power = power * u
    return total


def invert(mom):
    inv0 = 1.0 / mom[0]
    a0 = mom[1] * inv0
    s1 = [None] + [mom[l + 1] - a0 * mom[l] for l in range(1, 5)]
    inv1 = 1.0 / s1[1]
    quot = s1[2] * inv1
    a1 = quot - a0
    b1 = s1[1] * inv0
    s2_two = s1[3] - a1 * s1[2] - b1 * mom[2]
    s2_three = s1[4] - a1 * s1[3] - b1 * mom[3]
    a2 = s2_three / s2_two - quot
    b2 = s2_two * inv1
    q = (a0 + a1 + a2) * (1.0 / 3.0)
    d0, d1, d2 = a0 - q, a1 - q, a2 - q
    square = (d0 * d0 + d1 * d1 + d2 * d2 + 2.0 * b1 + 2.0 * b2) * (1.0 / 6.0)
    p = jnp.sqrt(square)
    det = d0 * d1 * d2 - d0 * b2 - d2 * b1
    ratio = det / (2.0 * square * p)
    high = q + 2.0 * p * cos_third(ratio)
    low = q - 2.0 * p * cos_third(-ratio)
    middle = 3.0 * q - high - low
    both = b1 * b2
    scale = mom[0] * both
    nodes = []
    for value in (low, middle, high):
        e0 = value - a0
        e1 = (value - a1) * e0 - b1
        nodes.append((scale / (both + b2 * (e0 * e0) + e1 * e1), value))
    return nodes


def write_sides(w, u, xup, xdn, yup, ydn, zs, lane):
    zs[0, 0:3] = w[:, :, 63, :]
    zs[0, 3:6] = u[:, :, 63, :]
    zs[0, 6:9] = w[:, :, 62, :]
    zs[1, 0:3] = w[:, :, 0, :]
    zs[1, 3:6] = u[:, :, 0, :]
    zs[1, 6:9] = w[:, :, 1, :]

    def rows(i, carry):
        z = pl.ds(pl.multiple_of(i * ROWS, ROWS), ROWS)
        xup[0:3, z, :] = w[:, 3, z, :]
        xup[3:6, z, :] = u[:, 3, z, :]
        xup[6:9, z, :] = w[:, 2, z, :]
        xdn[0:3, z, :] = w[:, 0, z, :]
        xdn[3:6, z, :] = u[:, 0, z, :]
        xdn[6:9, z, :] = w[:, 1, z, :]
        up = jnp.zeros((ROWS, 128), jnp.float32)
        dn = up
        for n in range(3):
            for x in range(4):
                vw, vu = w[n, x, z, :], u[n, x, z, :]
                for k, value, ahead, back in ((n, vw, 127, 0), (3 + n, vu, 127, 0), (6 + n, vw, 126, 1)):
                    at = 4 * k + x
                    up = jnp.where(lane == at, pltpu.roll(value, (at - ahead) % 128, 1), up)
                    dn = jnp.where(lane == at, pltpu.roll(value, (at - back) % 128, 1), dn)
        yup[z, :] = up
        ydn[z, :] = dn
        return carry

    lax.fori_loop(0, 64 // ROWS, rows, 0)


def lanes():
    return lax.broadcasted_iota(jnp.int32, (ROWS, 128), 1)


def write_top(top, mx):
    mx[...] = jnp.full(mx.shape, jnp.max(top), jnp.float32)


def step_of(received):
    top = jnp.max(received[...], axis=0, keepdims=True)
    return COURANT / (SPEED_TOTAL * top)


def entry_kernel(w, u, xup, xdn, yup, ydn, zs, mx):
    top = jnp.zeros((ROWS, 128), jnp.float32)
    for x in range(4):
        for i in range(64 // ROWS):
            z = slice(i * ROWS, (i + 1) * ROWS)
            top = jnp.maximum(top, jnp.maximum(jnp.abs(u[0, x, z, :]), jnp.maximum(jnp.abs(u[1, x, z, :]), jnp.abs(u[2, x, z, :]))))
    write_top(top, mx)
    write_sides(w, u, xup, xdn, yup, ydn, zs, lanes())


def middle_kernel(w, u, xlo, xhi, ylo, yhi, zr, got, base, mw, mu, xup, xdn, yup, ydn, zs, mx, pw, pu):
    f = Fields(w, u, pw, pu, xlo, xhi, ylo, yhi)
    pad_rows(f, zr)
    step = step_of(got)
    lane = lanes()

    def rows(i, top):
        z = pl.ds(pl.multiple_of(i * ROWS, ROWS), ROWS)
        for x in range(4):
            change, nodes = divergence(f, i, x, lane)
            start = moments_of(nodes)
            mid = [s - step * d for s, d in zip(start, change)]
            for k in range(6):
                base[k, x, z, :] = 0.5 * (start[k] + mid[k])
            for n, (weight, speed) in enumerate(invert(mid)):
                mw[n, x, z, :] = weight
                mu[n, x, z, :] = speed
                top = jnp.maximum(top, jnp.abs(speed))
        return top

    top = lax.fori_loop(0, 64 // ROWS, rows, jnp.zeros((ROWS, 128), jnp.float32))
    write_top(top, mx)
    write_sides(mw, mu, xup, xdn, yup, ydn, zs, lane)


def exit_kernel(w, u, xlo, xhi, ylo, yhi, zr, got, base, out, pw, pu):
    f = Fields(w, u, pw, pu, xlo, xhi, ylo, yhi)
    pad_rows(f, zr)
    half = 0.5 * step_of(got)
    lane = lanes()

    def rows(i, carry):
        z = pl.ds(pl.multiple_of(i * ROWS, ROWS), ROWS)
        for x in range(4):
            change, _ = divergence(f, i, x, lane)
            for k in range(6):
                out[k, x, z, :] = base[k, x, z, :] - half * change[k]
        return carry

    lax.fori_loop(0, 64 // ROWS, rows, 0)


def f32(*shape):
    return jax.ShapeDtypeStruct(shape, jnp.float32)


SIDES = (f32(9, 64, 128), f32(9, 64, 128), f32(64, 128), f32(64, 128), f32(2, 9, 4, 128))
NODES = (f32(3, 4, 64, 128), f32(3, 4, 64, 128))
PADDED = [pltpu.VMEM((3, 4, 80, 128), jnp.float32)] * 2


def call(kernel, outs, args, scratch=()):
    spec = pl.BlockSpec(memory_space=pltpu.VMEM)
    return pl.pallas_call(
        kernel,
        out_shape=outs,
        in_specs=[spec] * len(args),
        out_specs=jax.tree.map(lambda _: spec, outs),
        scratch_shapes=list(scratch),
        compiler_params=pltpu.CompilerParams(vmem_limit_bytes=24 * 1024 * 1024),
    )(*args)


def local(weights, abscissas):
    nx, ny, nz = (lax.axis_size(a) for a in AXES)
    everyone = nx * ny * nz

    def ring(n, s):
        return [(i, (i + s) % n) for i in range(n)]

    def exchange(xup, xdn, yup, ydn, zs):
        return (
            lax.ppermute(xup, "gx", ring(nx, 1)),
            lax.ppermute(xdn, "gx", ring(nx, -1)),
            lax.ppermute(yup, "gy", ring(ny, 1)),
            lax.ppermute(ydn, "gy", ring(ny, -1)),
            lax.ppermute(zs, "gz", ring(nz, 1)),
        )

    def spread(top):
        return lax.all_to_all(top.reshape(everyone, 1, 128), AXES, 0, 0).reshape(everyone, 128)

    tops = f32(everyone, 128)
    *sides, top = call(entry_kernel, SIDES + (tops,), (weights, abscissas))
    halo = exchange(*sides)
    got = spread(top)
    base, mw, mu, *sides, top = call(
        middle_kernel, (f32(6, 4, 64, 128),) + NODES + SIDES + (tops,),
        (weights, abscissas, *halo, got), PADDED)
    halo = exchange(*sides)
    got = spread(top)
    return call(exit_kernel, f32(6, 4, 64, 128), (mw, mu, *halo, got, base), PADDED)


def solution(mesh):
    spec = P(None, "gx", "gz", "gy")
    return jax.shard_map(local, mesh=mesh, in_specs=(spec, spec), out_specs=spec, check_vma=False)
```

```python
import numpy as np
import jax
import jax.numpy as jnp
from jax import lax
from jax.experimental import pallas as pl
from jax.experimental.pallas import tpu as pltpu
from jax.sharding import PartitionSpec as P


ENTRY_LIMIT = 53 * 1024 * 1024
COURANT = 0.4
SPEED_TOTAL = 1.72
SPEED_X, SPEED_Z, SPEED_Y = 0.6, 0.64, 0.48
ROWS = 8


def root_table(degree):
    points = np.cos((np.arange(400) + 0.5) * np.pi / 400)
    values = np.cos(2.0 / 3.0 * np.arccos(0.5 * (points + 1.0)))
    fit = np.polynomial.chebyshev.Chebyshev.fit(points, values, degree, domain=[-1, 1])
    return [float(c) for c in fit.convert(kind=np.polynomial.Polynomial).coef]


ROOT = root_table(11)


def cos_third(ratio):
    half = jnp.sqrt(jnp.maximum(0.5 + 0.5 * ratio, 0.0))
    t = 2.0 * half - 1.0
    total = jnp.full_like(t, ROOT[-1])
    for c in ROOT[-2::-1]:
        total = total * t + c
    return total


def limited(a, b):
    return jnp.maximum(jnp.minimum(a, b), 0.0) + jnp.minimum(jnp.maximum(a, b), 0.0)


def side_terms(c, wm2, wm1, w, wp1, wp2, um1, u, up1):
    d0, d1, d2, d3 = wm1 - wm2, w - wm1, wp1 - w, wp2 - wp1
    below = limited(d0, d1)
    here = (0.5 * c) * limited(d1, d2)
    above = limited(d2, d3)
    base = c * w
    own = (base + here) * jnp.maximum(u, 0.0) - (base - here) * jnp.minimum(u, 0.0)
    low = (wm1 + 0.5 * below) * (c * jnp.minimum(-um1, 0.0))
    high = (wp1 - 0.5 * above) * (c * jnp.minimum(up1, 0.0))
    return own, low, high


def odd_along(axis):
    return lax.rem(lax.axis_index(axis), 2)


def plane_at(x, odd):
    return x + odd * (3 - 2 * x)


class Nodes:
    def __init__(self, a, b, inner):
        self.a, self.b, self.inner = a, b, inner

    def w(self, n, x):
        return (self.a if x >= 2 else self.b).at[n if x in (0, 3) else 6 + n]

    def u(self, n, x):
        if x in (0, 3):
            return (self.a if x == 3 else self.b).at[3 + n]
        return self.inner.at[n if x == 2 else 3 + n]


class Fields(Nodes):
    def __init__(self, a, b, inner, xa, xb, ya, yb, pw, pu):
        super().__init__(a, b, inner)
        self.xa, self.xb, self.ya, self.yb, self.pw, self.pu = xa, xb, ya, yb, pw, pu
        self.sign = 1.0 - 2.0 * odd_along("gx").astype(jnp.float32)
        self.y_odd = odd_along("gy")

    def plane_w(self, n, x):
        if x in (-1, 4):
            return (self.xa if x == 4 else self.xb).at[n]
        if x in (-2, 5):
            return (self.xa if x == 5 else self.xb).at[6 + n]
        return self.w(n, x)

    def plane_u(self, n, x):
        if x in (-1, 4):
            return (self.xa if x == 4 else self.xb).at[3 + n]
        return self.u(n, x)


def pad_rows(f, zr):
    def copy(i, carry):
        z = pl.ds(pl.multiple_of(i * ROWS, ROWS), ROWS)
        zp = pl.ds(pl.multiple_of(i * ROWS + 8, ROWS), ROWS)
        for n in range(3):
            for x in range(4):
                f.pw[n, x, zp, :] = f.w(n, x)[z, :]
                f.pu[n, x, zp, :] = f.u(n, x)[z, :]
        return carry

    lax.fori_loop(0, 64 // ROWS, copy, 0)
    f.pw[:, :, 7, :] = zr[0, 0:3]
    f.pu[:, :, 7, :] = zr[0, 3:6]
    f.pw[:, :, 6, :] = zr[0, 6:9]
    f.pw[:, :, 72, :] = zr[1, 0:3]
    f.pu[:, :, 72, :] = zr[1, 3:6]
    f.pw[:, :, 73, :] = zr[1, 6:9]


def divergence(f, i, x, lane):
    z0 = i * ROWS
    z = pl.ds(pl.multiple_of(z0, ROWS), ROWS)
    first, final = lane == 0, lane == 127
    flip = f.y_odd == 1
    ha, hb = f.ya[z, :], f.yb[z, :]
    hlo, hhi = jnp.where(flip, ha, hb), jnp.where(flip, hb, ha)

    def halo_lo(k):
        return pltpu.roll(hlo, (128 - (4 * k + x)) % 128, 1)

    def halo_hi(k):
        return pltpu.roll(hhi, 127 - (4 * k + x), 1)

    total = [None] * 6
    for n in range(3):
        w, u = f.w(n, x)[z, :], f.u(n, x)[z, :]
        parts = []
        um1, up1 = f.plane_u(n, x - 1)[z, :], f.plane_u(n, x + 1)[z, :]
        own, low, high = side_terms(
            SPEED_X, *[f.plane_w(n, x + s)[z, :] for s in (-2, -1)], w,
            *[f.plane_w(n, x + s)[z, :] for s in (1, 2)], f.sign * um1, f.sign * u, f.sign * up1)
        parts += [(low, um1), (high, up1)]

        def row_w(s):
            return f.pw[n, x, pl.ds(z0 + 8 + s, ROWS), :]

        um1, up1 = f.pu[n, x, pl.ds(z0 + 7, ROWS), :], f.pu[n, x, pl.ds(z0 + 9, ROWS), :]
        own_z, low, high = side_terms(
            SPEED_Z, row_w(-2), row_w(-1), w, row_w(1), row_w(2), um1, u, up1)
        parts += [(low, um1), (high, up1)]
        own = own + own_z
        um1 = jnp.where(first, halo_lo(3 + n), pltpu.roll(u, 1, 1))
        up1 = jnp.where(final, halo_hi(3 + n), pltpu.roll(u, 127, 1))
        wm1 = jnp.where(first, halo_lo(n), pltpu.roll(w, 1, 1))
        wp1 = jnp.where(final, halo_hi(n), pltpu.roll(w, 127, 1))
        wm2 = jnp.where(first, halo_lo(6 + n), pltpu.roll(wm1, 1, 1))
        wp2 = jnp.where(final, halo_hi(6 + n), pltpu.roll(wp1, 127, 1))
        own_y, low, high = side_terms(SPEED_Y, wm2, wm1, w, wp1, wp2, um1, u, up1)
        parts += [(low, um1), (high, up1)]
        own = own + own_y
        parts.append((own, u))
        for order in range(6):
            term = parts[0][0]
            for value, _ in parts[1:]:
                term = term + value
            total[order] = term if total[order] is None else total[order] + term
            if order < 5:
                parts = [(value * speed, speed) for value, speed in parts]
    return total


def moments_of(nodes):
    total = [None] * 6
    for w, u in nodes:
        power = w
        for order in range(6):
            total[order] = power if total[order] is None else total[order] + power
            if order < 5:
                power = power * u
    return total


def invert(mom):
    inv0 = 1.0 / mom[0]
    a0 = mom[1] * inv0
    s1 = [None] + [mom[l + 1] - a0 * mom[l] for l in range(1, 5)]
    inv1 = 1.0 / s1[1]
    quot = s1[2] * inv1
    a1 = quot - a0
    b1 = s1[1] * inv0
    s2_two = s1[3] - a1 * s1[2] - b1 * mom[2]
    s2_three = s1[4] - a1 * s1[3] - b1 * mom[3]
    a2 = s2_three / s2_two - quot
    b2 = s2_two * inv1
    q = (a0 + a1 + a2) * (1.0 / 3.0)
    d0, d1, d2 = a0 - q, a1 - q, a2 - q
    square = (d0 * d0 + d1 * d1 + d2 * d2 + 2.0 * b1 + 2.0 * b2) * (1.0 / 6.0)
    p = jnp.sqrt(square)
    det = d0 * d1 * d2 - d0 * b2 - d2 * b1
    ratio = det / (2.0 * square * p)
    high = q + 2.0 * p * cos_third(ratio)
    low = q - 2.0 * p * cos_third(-ratio)
    middle = 3.0 * q - high - low
    both = b1 * b2
    scale = mom[0] * both
    nodes = []
    for value in (low, middle, high):
        e0 = value - a0
        e1 = (value - a1) * e0 - b1
        nodes.append((scale / (both + b2 * (e0 * e0) + e1 * e1), value))
    return nodes


def lanes():
    return lax.broadcasted_iota(jnp.int32, (ROWS, 128), 1)


def rows_of(i):
    return pl.ds(pl.multiple_of(i * ROWS, ROWS), ROWS)


def write_top(top, mx):
    mx[...] = jnp.full(mx.shape, jnp.max(top), jnp.float32)


def step_of(received):
    top = jnp.max(received[...], axis=0, keepdims=True)
    return COURANT / (SPEED_TOTAL * top)


def relay_kernel(got, mx):
    mx[...] = jnp.broadcast_to(jnp.max(got[...], axis=0, keepdims=True), mx.shape)


def entry_kernel(w, u, a, b, inner, mx, sems):
    nodes = Nodes(a, b, inner)
    odd = odd_along("gx")
    loads = [
        pltpu.make_async_copy(array.at[n, plane_at(x, odd)], side(n, x), sems.at[at, n, x])
        for at, (array, side) in enumerate(((u, nodes.u), (w, nodes.w)))
        for n in range(3) for x in range(4)
    ]
    for copy in loads:
        copy.start()
    top = jnp.zeros((ROWS, 128), jnp.float32)
    for at in range(12):
        loads[at].wait()
        for i in range(64 // ROWS):
            top = jnp.maximum(top, jnp.abs(nodes.u(at // 4, at % 4)[i * ROWS:(i + 1) * ROWS, :]))
    write_top(top, mx)
    for copy in loads[12:]:
        copy.wait()


def edge_kernel(a, b, inner, ya, yb, zs):
    nodes = Nodes(a, b, inner)
    lane = lanes()
    flip = odd_along("gy") == 1
    for n in range(3):
        for x in range(4):
            w, u = nodes.w(n, x), nodes.u(n, x)
            for k, row, other, side in ((n, 63, 0, w), (3 + n, 63, 0, u), (6 + n, 62, 1, w)):
                zs[0, k, x, :] = side[row, :]
                zs[1, k, x, :] = side[other, :]

    def rows(i, carry):
        z = rows_of(i)
        up = jnp.zeros((ROWS, 128), jnp.float32)
        dn = up
        for n in range(3):
            for x in range(4):
                vw, vu = nodes.w(n, x)[z, :], nodes.u(n, x)[z, :]
                for k, value, ahead, back in ((n, vw, 127, 0), (3 + n, vu, 127, 0), (6 + n, vw, 126, 1)):
                    at = 4 * k + x
                    up = jnp.where(lane == at, pltpu.roll(value, (at - ahead) % 128, 1), up)
                    dn = jnp.where(lane == at, pltpu.roll(value, (at - back) % 128, 1), dn)
        ya[z, :] = jnp.where(flip, dn, up)
        yb[z, :] = jnp.where(flip, up, dn)
        return carry

    lax.fori_loop(0, 64 // ROWS, rows, 0)


def change_kernel(a, b, inner, xa, xb, ya, yb, zr, out, pw, pu):
    f = Fields(a, b, inner, xa, xb, ya, yb, pw, pu)
    pad_rows(f, zr)
    lane = lanes()

    def rows(i, carry):
        for x in range(4):
            for k, value in enumerate(divergence(f, i, x, lane)):
                out[k, x, rows_of(i), :] = value
        return carry

    lax.fori_loop(0, 64 // ROWS, rows, 0)


def middle_kernel(change, a, b, inner, got, base, mid_a, mid_b, mid_inner, mx):
    step = step_of(got)
    old, new = Nodes(a, b, inner), Nodes(mid_a, mid_b, mid_inner)

    def rows(i, top):
        z = rows_of(i)
        for x in range(4):
            mid = []
            for k, moment in enumerate(moments_of([(old.w(n, x)[z, :], old.u(n, x)[z, :]) for n in range(3)])):
                mid.append(moment - step * change[k, x, z, :])
                base[k, x, z, :] = 0.5 * (moment + mid[k])
            for n, (weight, speed) in enumerate(invert(mid)):
                new.w(n, x)[z, :] = weight
                new.u(n, x)[z, :] = speed
                top = jnp.maximum(top, jnp.abs(speed))
        return top

    top = lax.fori_loop(0, 64 // ROWS, rows, jnp.zeros((ROWS, 128), jnp.float32))
    write_top(top, mx)


def exit_kernel(change, base, got, out, held, sems):
    half = 0.5 * step_of(got)
    odd = odd_along("gx")
    stores = []
    for k in range(6):
        for x in range(4):
            held[k, x] = base[k, x] - half * change[k, x]
            stores.append(pltpu.make_async_copy(held.at[k, x], out.at[k, plane_at(x, odd)], sems.at[k, x]))
            stores[-1].start()
    for copy in stores:
        copy.wait()


def f32(*shape):
    return jax.ShapeDtypeStruct(shape, jnp.float32)


PLANES = (f32(9, 64, 128), f32(9, 64, 128), f32(6, 64, 128))
EDGES = (f32(64, 128), f32(64, 128), f32(2, 9, 4, 128))
MOMENTS = f32(6, 4, 64, 128)
PADDED = [pltpu.VMEM((3, 4, 80, 128), jnp.float32)] * 2
VM = pl.BlockSpec(memory_space=pltpu.VMEM)
ANY = pl.BlockSpec(memory_space=pltpu.HBM)


def call(kernel, outs, args, scratch=(), ins=VM, out=VM, flops=1, limit=8 * 1024 * 1024):
    return pl.pallas_call(
        kernel,
        out_shape=outs,
        in_specs=[ins] * len(args),
        out_specs=out if isinstance(out, tuple) else jax.tree.map(lambda _: out, outs),
        scratch_shapes=list(scratch),
        cost_estimate=pl.CostEstimate(flops=flops, bytes_accessed=1 << 20, transcendentals=0),
        compiler_params=pltpu.CompilerParams(vmem_limit_bytes=limit),
    )(*args)


def pairs(n, first):
    return [(i, (i + 1) % n) for i in range(first, n, 2)] + [((i + 1) % n, i) for i in range(first, n, 2)]


def local(weights, abscissas):
    nx, ny, nz = (lax.axis_size(a) for a in ("gx", "gy", "gz"))
    swap = [(i, (i + 1) % nz) for i in range(nz)]

    def exchange(xa, xb, ya, yb, zs):
        return (
            lax.ppermute(xa, "gx", pairs(nx, 0)),
            lax.ppermute(xb, "gx", pairs(nx, 1)),
            lax.ppermute(ya, "gy", pairs(ny, 0)),
            lax.ppermute(yb, "gy", pairs(ny, 1)),
            lax.ppermute(zs, "gz", swap),
        )

    def spread(top, axes, n):
        return lax.all_to_all(top.reshape(n, 1, 128), axes, 0, 0).reshape(n, 128)

    def largest(top):
        got = spread(top, ("gy", "gz"), ny * nz)
        top = call(relay_kernel, f32(nx, 128), (got,))
        return spread(top, ("gx",), nx)

    tops = f32(ny * nz, 128)
    *planes, top = call(
        entry_kernel, PLANES + (tops,), (weights, abscissas),
        [pltpu.SemaphoreType.DMA((2, 3, 4))], ins=ANY, limit=ENTRY_LIMIT)
    edges = call(edge_kernel, EDGES, planes, flops=2 << 20)
    halo = exchange(*planes[:2], *edges)
    got = largest(top)
    change = call(change_kernel, MOMENTS, (*planes, *halo), PADDED, flops=4 << 20)
    base, *planes, top = call(
        middle_kernel, (MOMENTS,) + PLANES + (tops,), (change, *planes, got), flops=4 << 20)
    edges = call(edge_kernel, EDGES, planes, flops=2 << 20)
    halo = exchange(*planes[:2], *edges)
    got = largest(top)
    change = call(change_kernel, MOMENTS, (*planes, *halo), PADDED, flops=4 << 20)
    return call(
        exit_kernel, MOMENTS, (change, base, got),
        [pltpu.VMEM((6, 4, 64, 128), jnp.float32), pltpu.SemaphoreType.DMA((6, 4))], out=ANY)


def solution(mesh):
    spec = P(None, "gx", "gz", "gy")
    return jax.shard_map(local, mesh=mesh, in_specs=(spec, spec), out_specs=spec, check_vma=False)
```

```python
import numpy as np
import jax
import jax.numpy as jnp
from jax import lax
from jax.experimental import pallas as pl
from jax.experimental.pallas import tpu as pltpu
from jax.sharding import PartitionSpec as P


ENTRY_LIMIT = 53 * 1024 * 1024
COURANT = 0.4
SPEED_TOTAL = 1.72
SPEED_X, SPEED_Z, SPEED_Y = 0.6, 0.64, 0.48
ROWS = 8


def root_table(degree):
    points = np.cos((np.arange(400) + 0.5) * np.pi / 400)
    values = np.cos(2.0 / 3.0 * np.arccos(0.5 * (points + 1.0)))
    fit = np.polynomial.chebyshev.Chebyshev.fit(points, values, degree, domain=[-1, 1])
    return [float(c) for c in fit.convert(kind=np.polynomial.Polynomial).coef]


ROOT = root_table(11)


def cos_third(ratio):
    half = jnp.sqrt(jnp.maximum(0.5 + 0.5 * ratio, 0.0))
    t = 2.0 * half - 1.0
    total = jnp.full_like(t, ROOT[-1])
    for c in ROOT[-2::-1]:
        total = total * t + c
    return total


def limited(a, b):
    return jnp.maximum(jnp.minimum(a, b), 0.0) + jnp.minimum(jnp.maximum(a, b), 0.0)


def side_terms(c, wm2, wm1, w, wp1, wp2, um1, u, up1):
    d0, d1, d2, d3 = wm1 - wm2, w - wm1, wp1 - w, wp2 - wp1
    below = limited(d0, d1)
    here = (0.5 * c) * limited(d1, d2)
    above = limited(d2, d3)
    base = c * w
    own = (base + here) * jnp.maximum(u, 0.0) - (base - here) * jnp.minimum(u, 0.0)
    low = (wm1 + 0.5 * below) * (c * jnp.minimum(-um1, 0.0))
    high = (wp1 - 0.5 * above) * (c * jnp.minimum(up1, 0.0))
    return own, low, high


def odd_along(axis):
    return lax.rem(lax.axis_index(axis), 2)


def plane_at(x, odd):
    return x + odd * (3 - 2 * x)


class Nodes:
    def __init__(self, a, b, inner):
        self.a, self.b, self.inner = a, b, inner

    def w(self, n, x):
        return (self.a if x >= 2 else self.b).at[n if x in (0, 3) else 6 + n]

    def u(self, n, x):
        if x in (0, 3):
            return (self.a if x == 3 else self.b).at[3 + n]
        return self.inner.at[n if x == 2 else 3 + n]


def rows_of(i):
    return pl.ds(pl.multiple_of(i * ROWS, ROWS), ROWS)


def add_powers(total, parts):
    done = []
    for order in range(6):
        term = parts[0][0]
        for value, _ in parts[1:]:
            term = term + value
        done.append(term if total is None else total[order] + term)
        if order < 5:
            parts = [(value * speed, speed) for value, speed in parts]
    return done


def cross_kernel(a, b, inner, xa, xb, zr, out, pw, pu):
    nodes, sign = Nodes(a, b, inner), 1.0 - 2.0 * odd_along("gx").astype(jnp.float32)

    def plane_w(n, x):
        if x in (-1, 4):
            return (xa if x == 4 else xb).at[n]
        if x in (-2, 5):
            return (xa if x == 5 else xb).at[6 + n]
        return nodes.w(n, x)

    def plane_u(n, x):
        if x in (-1, 4):
            return (xa if x == 4 else xb).at[3 + n]
        return nodes.u(n, x)

    def copy(i, carry):
        zp = pl.ds(pl.multiple_of(i * ROWS + 8, ROWS), ROWS)
        for n in range(3):
            for x in range(4):
                pw[n, x, zp, :] = nodes.w(n, x)[rows_of(i), :]
                pu[n, x, zp, :] = nodes.u(n, x)[rows_of(i), :]
        return carry

    lax.fori_loop(0, 64 // ROWS, copy, 0)
    pw[:, :, 7, :] = zr[0, 0:3]
    pu[:, :, 7, :] = zr[0, 3:6]
    pw[:, :, 6, :] = zr[0, 6:9]
    pw[:, :, 72, :] = zr[1, 0:3]
    pu[:, :, 72, :] = zr[1, 3:6]
    pw[:, :, 73, :] = zr[1, 6:9]

    def rows(i, carry):
        z = rows_of(i)
        for x in range(4):
            total = None
            for n in range(3):
                w, u = nodes.w(n, x)[z, :], nodes.u(n, x)[z, :]
                um1, up1 = plane_u(n, x - 1)[z, :], plane_u(n, x + 1)[z, :]
                own, low, high = side_terms(
                    SPEED_X, plane_w(n, x - 2)[z, :], plane_w(n, x - 1)[z, :], w,
                    plane_w(n, x + 1)[z, :], plane_w(n, x + 2)[z, :], sign * um1, sign * u, sign * up1)
                parts = [(low, um1), (high, up1)]

                def row(ref, s):
                    return ref[n, x, pl.ds(i * ROWS + 8 + s, ROWS), :]

                um1, up1 = row(pu, -1), row(pu, 1)
                own_z, low, high = side_terms(
                    SPEED_Z, row(pw, -2), row(pw, -1), w, row(pw, 1), row(pw, 2), um1, u, up1)
                parts += [(low, um1), (high, up1), (own + own_z, u)]
                total = add_powers(total, parts)
            for k in range(6):
                out[k, x, z, :] = total[k]
        return carry

    lax.fori_loop(0, 64 // ROWS, rows, 0)


def along_kernel(change, a, b, inner, ya, yb, out):
    nodes, flip, lane = Nodes(a, b, inner), odd_along("gy") == 1, lanes()
    first, final = lane == 0, lane == 127

    def rows(i, carry):
        z = rows_of(i)
        va, vb = ya[z, :], yb[z, :]
        below, above = jnp.where(flip, va, vb), jnp.where(flip, vb, va)
        edge = jnp.where(lane % 4 >= 2, above, pltpu.roll(below, 4, 1))
        for x in range(4):
            total = [change[k, x, z, :] for k in range(6)]
            for n in range(3):
                w, u = nodes.w(n, x)[z, :], nodes.u(n, x)[z, :]
                outer = pltpu.roll(edge, 124 - 4 * (3 * x + n), 1)
                wm2 = jnp.where(lane < 2, outer, pltpu.roll(w, 2, 1))
                wp2 = jnp.where(lane >= 126, outer, pltpu.roll(w, 126, 1))
                wm1 = jnp.where(first, pltpu.roll(outer, 127, 1), pltpu.roll(w, 1, 1))
                wp1 = jnp.where(final, pltpu.roll(outer, 1, 1), pltpu.roll(w, 127, 1))
                at = 48 + 2 * (3 * x + n)
                um1 = jnp.where(first, pltpu.roll(below, 128 - at, 1), pltpu.roll(u, 1, 1))
                up1 = jnp.where(final, pltpu.roll(above, 126 - at, 1), pltpu.roll(u, 127, 1))
                own, low, high = side_terms(SPEED_Y, wm2, wm1, w, wp1, wp2, um1, u, up1)
                total = add_powers(total, [(low, um1), (high, up1), (own, u)])
            for k in range(6):
                out[k, x, z, :] = total[k]
        return carry

    lax.fori_loop(0, 64 // ROWS, rows, 0)


def moments_of(nodes):
    total = [None] * 6
    for w, u in nodes:
        power = w
        for order in range(6):
            total[order] = power if total[order] is None else total[order] + power
            if order < 5:
                power = power * u
    return total


def invert(mom):
    inv0 = 1.0 / mom[0]
    a0 = mom[1] * inv0
    s1 = [None] + [mom[l + 1] - a0 * mom[l] for l in range(1, 5)]
    inv1 = 1.0 / s1[1]
    quot = s1[2] * inv1
    a1 = quot - a0
    b1 = s1[1] * inv0
    s2_two = s1[3] - a1 * s1[2] - b1 * mom[2]
    s2_three = s1[4] - a1 * s1[3] - b1 * mom[3]
    a2 = s2_three / s2_two - quot
    b2 = s2_two * inv1
    q = (a0 + a1 + a2) * (1.0 / 3.0)
    d0, d1, d2 = a0 - q, a1 - q, a2 - q
    square = (d0 * d0 + d1 * d1 + d2 * d2 + 2.0 * b1 + 2.0 * b2) * (1.0 / 6.0)
    p = jnp.sqrt(square)
    det = d0 * d1 * d2 - d0 * b2 - d2 * b1
    ratio = det / (2.0 * square * p)
    high = q + 2.0 * p * cos_third(ratio)
    low = q - 2.0 * p * cos_third(-ratio)
    middle = 3.0 * q - high - low
    both = b1 * b2
    scale = mom[0] * both
    nodes = []
    for value in (low, middle, high):
        e0 = value - a0
        e1 = (value - a1) * e0 - b1
        nodes.append((scale / (both + b2 * (e0 * e0) + e1 * e1), value))
    return nodes


def lanes():
    return lax.broadcasted_iota(jnp.int32, (ROWS, 128), 1)


def write_top(top, mx):
    mx[...] = jnp.full(mx.shape, jnp.max(top), jnp.float32)


def step_of(received):
    top = jnp.max(received[...], axis=0, keepdims=True)
    return COURANT / (SPEED_TOTAL * top)


def relay_kernel(got, mx):
    mx[...] = jnp.broadcast_to(jnp.max(got[...], axis=0, keepdims=True), mx.shape)


def entry_kernel(w, u, a, b, inner, zs, mx, sems):
    nodes = Nodes(a, b, inner)
    odd = odd_along("gx")
    loads = [
        pltpu.make_async_copy(array.at[n, plane_at(x, odd)], side(n, x), sems.at[at, n, x])
        for at, (array, side) in enumerate(((u, nodes.u), (w, nodes.w)))
        for n in range(3) for x in range(4)
    ]
    for copy in loads:
        copy.start()
    top = jnp.zeros((ROWS, 128), jnp.float32)
    for at in range(12):
        loads[at].wait()
        for i in range(64 // ROWS):
            top = jnp.maximum(top, jnp.abs(nodes.u(at // 4, at % 4)[i * ROWS:(i + 1) * ROWS, :]))
    write_top(top, mx)
    for copy in loads[12:]:
        copy.wait()
    write_rows(nodes, zs)


def write_rows(nodes, zs):
    for n in range(3):
        for x in range(4):
            w, u = nodes.w(n, x), nodes.u(n, x)
            for k, side, top, bottom in ((n, w, 63, 0), (3 + n, u, 63, 0), (6 + n, w, 62, 1)):
                zs[0, k, x, :] = side[top, :]
                zs[1, k, x, :] = side[bottom, :]


def edge_kernel(a, b, inner, ys):
    nodes, lane = Nodes(a, b, inner), lanes()

    def rows(i, carry):
        z = rows_of(i)
        packed = jnp.zeros((ROWS, 128), jnp.float32)
        for x in range(4):
            for n in range(3):
                at = 3 * x + n
                packed = jnp.where(lane // 4 == at, pltpu.roll(nodes.w(n, x)[z, :], 4 * at + 2, 1), packed)
                packed = jnp.where(lane // 2 == 24 + at, pltpu.roll(nodes.u(n, x)[z, :], 49 + 2 * at, 1), packed)
        ys[z, :] = packed
        return carry

    lax.fori_loop(0, 64 // ROWS, rows, 0)


def middle_kernel(change, a, b, inner, got, base, mid_a, mid_b, mid_inner, zs, mx):
    step = step_of(got)
    old, new = Nodes(a, b, inner), Nodes(mid_a, mid_b, mid_inner)

    def rows(i, top):
        z = rows_of(i)
        for x in range(4):
            mid = []
            for k, moment in enumerate(moments_of([(old.w(n, x)[z, :], old.u(n, x)[z, :]) for n in range(3)])):
                mid.append(moment - step * change[k, x, z, :])
                base[k, x, z, :] = 0.5 * (moment + mid[k])
            for n, (weight, speed) in enumerate(invert(mid)):
                new.w(n, x)[z, :] = weight
                new.u(n, x)[z, :] = speed
                top = jnp.maximum(top, jnp.abs(speed))
        return top

    top = lax.fori_loop(0, 64 // ROWS, rows, jnp.zeros((ROWS, 128), jnp.float32))
    write_top(top, mx)
    write_rows(new, zs)


def exit_kernel(change, base, got, out, held, sems):
    half = 0.5 * step_of(got)
    odd = odd_along("gx")
    stores = []
    for k in range(6):
        for x in range(4):
            held[k, x] = base[k, x] - half * change[k, x]
            stores.append(pltpu.make_async_copy(held.at[k, x], out.at[k, plane_at(x, odd)], sems.at[k, x]))
            stores[-1].start()
    for copy in stores:
        copy.wait()


def f32(*shape):
    return jax.ShapeDtypeStruct(shape, jnp.float32)


PLANES = (f32(9, 64, 128), f32(9, 64, 128), f32(6, 64, 128))
ROWS_Z = f32(2, 9, 4, 128)
MOMENTS = f32(6, 4, 64, 128)
PADDED = [pltpu.VMEM((3, 4, 80, 128), jnp.float32)] * 2
VM = pl.BlockSpec(memory_space=pltpu.VMEM)
ANY = pl.BlockSpec(memory_space=pltpu.HBM)


def call(kernel, outs, args, scratch=(), ins=VM, out=VM, flops=1, limit=8 * 1024 * 1024):
    return pl.pallas_call(
        kernel,
        out_shape=outs,
        in_specs=[ins] * len(args),
        out_specs=out if isinstance(out, tuple) else jax.tree.map(lambda _: out, outs),
        scratch_shapes=list(scratch),
        cost_estimate=pl.CostEstimate(flops=flops, bytes_accessed=1 << 20, transcendentals=0),
        compiler_params=pltpu.CompilerParams(vmem_limit_bytes=limit),
    )(*args)


def pairs(n, first):
    return [(i, (i + 1) % n) for i in range(first, n, 2)] + [((i + 1) % n, i) for i in range(first, n, 2)]


def local(weights, abscissas):
    nx, ny, nz = (lax.axis_size(a) for a in ("gx", "gy", "gz"))
    swap = [(i, (i + 1) % nz) for i in range(nz)]

    def exchange(a, b, inner, zs):
        ys = call(edge_kernel, f32(64, 128), (a, b, inner), flops=1 << 20)
        return (
            lax.ppermute(a, "gx", pairs(nx, 0)),
            lax.ppermute(b, "gx", pairs(nx, 1)),
            lax.ppermute(zs, "gz", swap),
            lax.ppermute(ys, "gy", pairs(ny, 0)),
            lax.ppermute(ys, "gy", pairs(ny, 1)),
        )

    def change_of(planes, xa, xb, zr, ya, yb):
        change = call(cross_kernel, MOMENTS, (*planes, xa, xb, zr), PADDED, flops=4 << 20)
        return call(along_kernel, MOMENTS, (change, *planes, ya, yb), flops=2 << 20)

    def spread(top, axes, n):
        return lax.all_to_all(top.reshape(n, 1, 128), axes, 0, 0).reshape(n, 128)

    def largest(top):
        got = spread(top, ("gy", "gz"), ny * nz)
        top = call(relay_kernel, f32(nx, 128), (got,))
        return spread(top, ("gx",), nx)

    tops = f32(ny * nz, 128)
    *planes, zs, top = call(
        entry_kernel, PLANES + (ROWS_Z, tops), (weights, abscissas),
        [pltpu.SemaphoreType.DMA((2, 3, 4))], ins=ANY, limit=ENTRY_LIMIT)
    halo = exchange(*planes, zs)
    got = largest(top)
    change = change_of(planes, *halo)
    base, *planes, zs, top = call(
        middle_kernel, (MOMENTS,) + PLANES + (ROWS_Z, tops), (change, *planes, got), flops=4 << 20)
    halo = exchange(*planes, zs)
    got = largest(top)
    change = change_of(planes, *halo)
    return call(
        exit_kernel, MOMENTS, (change, base, got),
        [pltpu.VMEM((6, 4, 64, 128), jnp.float32), pltpu.SemaphoreType.DMA((6, 4))], out=ANY)


def solution(mesh):
    spec = P(None, "gx", "gz", "gy")
    return jax.shard_map(local, mesh=mesh, in_specs=(spec, spec), out_specs=spec, check_vma=False)
```

```python
import numpy as np
import jax
import jax.numpy as jnp
from jax import lax
from jax.experimental import pallas as pl
from jax.experimental.pallas import tpu as pltpu
from jax.sharding import PartitionSpec as P


ENTRY_LIMIT = 53 * 1024 * 1024
COURANT = 0.4
SPEED_TOTAL = 1.72
SPEED_X, SPEED_Z, SPEED_Y = 0.6, 0.64, 0.48
ROWS = 8
LONG = 32
EDGE = 64


def root_table(degree):
    points = np.cos((np.arange(400) + 0.5) * np.pi / 400)
    values = np.cos(2.0 / 3.0 * np.arccos(0.5 * (points + 1.0)))
    fit = np.polynomial.chebyshev.Chebyshev.fit(points, values, degree, domain=[-1, 1])
    return [float(c) for c in fit.convert(kind=np.polynomial.Polynomial).coef]


ROOT = root_table(11)


def cos_third(ratio):
    half = jnp.sqrt(jnp.maximum(0.5 + 0.5 * ratio, 0.0))
    t = 2.0 * half - 1.0
    total = jnp.full_like(t, ROOT[-1])
    for c in ROOT[-2::-1]:
        total = total * t + c
    return total


def limited(a, b):
    return jnp.maximum(jnp.minimum(a, b), 0.0) + jnp.minimum(jnp.maximum(a, b), 0.0)


def side_terms(c, wm2, wm1, w, wp1, wp2, um1, u, up1):
    d0, d1, d2, d3 = wm1 - wm2, w - wm1, wp1 - w, wp2 - wp1
    below = limited(d0, d1)
    here = (0.5 * c) * limited(d1, d2)
    above = limited(d2, d3)
    base = c * w
    own = (base + here) * jnp.maximum(u, 0.0) - (base - here) * jnp.minimum(u, 0.0)
    low = (wm1 + 0.5 * below) * (c * jnp.minimum(-um1, 0.0))
    high = (wp1 - 0.5 * above) * (c * jnp.minimum(up1, 0.0))
    return own, low, high


def odd_along(axis):
    return lax.rem(lax.axis_index(axis), 2)


def plane_at(x, odd):
    return x + odd * (3 - 2 * x)


class Nodes:
    def __init__(self, a, b, inner):
        self.a, self.b, self.inner = a, b, inner

    def w(self, n, x):
        return (self.a if x >= 2 else self.b).at[n if x in (0, 3) else 6 + n]

    def u(self, n, x):
        if x in (0, 3):
            return (self.a if x == 3 else self.b).at[3 + n]
        return self.inner.at[n if x == 2 else 3 + n]


def rows_of(i, rows=ROWS):
    return pl.ds(pl.multiple_of(i * rows, rows), rows)


def add_powers(total, parts):
    done = []
    for order in range(6):
        term = parts[0][0]
        for value, _ in parts[1:]:
            term = term + value
        done.append(term if total is None else total[order] + term)
        if order < 5:
            parts = [(value * speed, speed) for value, speed in parts]
    return done


def row_at(side, k, x):
    return 36 * side + 4 * k + x


def write_rows(nodes, top, zs, mx):
    most = jnp.full(mx.shape, jnp.max(top), jnp.float32)
    mx[...] = most
    zs[72:80, :] = most
    for n in range(3):
        for x in range(4):
            w, u = nodes.w(n, x), nodes.u(n, x)
            for k, side, top, bottom in ((n, w, 63, 0), (3 + n, u, 63, 0), (6 + n, w, 62, 1)):
                zs[row_at(0, k, x), :] = side[top, :]
                zs[row_at(1, k, x), :] = side[bottom, :]


def cross_kernel(a, b, inner, xa, xb, zr, out, pw, pu):
    nodes, sign = Nodes(a, b, inner), 1.0 - 2.0 * odd_along("gx").astype(jnp.float32)

    def plane_w(n, x):
        if x in (-1, 4):
            return (xa if x == 4 else xb).at[n]
        if x in (-2, 5):
            return (xa if x == 5 else xb).at[6 + n]
        return nodes.w(n, x)

    def plane_u(n, x):
        if x in (-1, 4):
            return (xa if x == 4 else xb).at[3 + n]
        return nodes.u(n, x)

    def copy(i, carry):
        zp = pl.ds(pl.multiple_of(i * ROWS + 8, ROWS), ROWS)
        for n in range(3):
            for x in range(4):
                pw[n, x, zp, :] = nodes.w(n, x)[rows_of(i), :]
                pu[n, x, zp, :] = nodes.u(n, x)[rows_of(i), :]
        return carry

    lax.fori_loop(0, 64 // ROWS, copy, 0)
    for n in range(3):
        for x in range(4):
            pw[n, x, 7, :] = zr[row_at(0, n, x), :]
            pu[n, x, 7, :] = zr[row_at(0, 3 + n, x), :]
            pw[n, x, 6, :] = zr[row_at(0, 6 + n, x), :]
            pw[n, x, 72, :] = zr[row_at(1, n, x), :]
            pu[n, x, 72, :] = zr[row_at(1, 3 + n, x), :]
            pw[n, x, 73, :] = zr[row_at(1, 6 + n, x), :]

    def rows(i, carry):
        z = rows_of(i)
        for x in range(4):
            total = None
            for n in range(3):
                w, u = nodes.w(n, x)[z, :], nodes.u(n, x)[z, :]
                um1, up1 = plane_u(n, x - 1)[z, :], plane_u(n, x + 1)[z, :]
                own, low, high = side_terms(
                    SPEED_X, plane_w(n, x - 2)[z, :], plane_w(n, x - 1)[z, :], w,
                    plane_w(n, x + 1)[z, :], plane_w(n, x + 2)[z, :], sign * um1, sign * u, sign * up1)
                parts = [(low, um1), (high, up1)]

                def row(ref, s):
                    return ref[n, x, pl.ds(i * ROWS + 8 + s, ROWS), :]

                um1, up1 = row(pu, -1), row(pu, 1)
                own_z, low, high = side_terms(
                    SPEED_Z, row(pw, -2), row(pw, -1), w, row(pw, 1), row(pw, 2), um1, u, up1)
                parts += [(low, um1), (high, up1), (own + own_z, u)]
                total = add_powers(total, parts)
            for k in range(6):
                out[k, x, z, :] = total[k]
        return carry

    lax.fori_loop(0, 64 // ROWS, rows, 0)


def along_kernel(change, a, b, inner, ya, yb, out):
    nodes, flip, lane = Nodes(a, b, inner), odd_along("gy") == 1, lanes(LONG)
    first, final = lane == 0, lane == 127

    def rows(i, carry):
        z = rows_of(i, LONG)
        va, vb = ya[z, :], yb[z, :]
        below, above = jnp.where(flip, va, vb), jnp.where(flip, vb, va)
        edge = jnp.where(lane % 4 >= 2, above, pltpu.roll(below, 4, 1))
        for x in range(4):
            total = [change[k, x, z, :] for k in range(6)]
            for n in range(3):
                w, u = nodes.w(n, x)[z, :], nodes.u(n, x)[z, :]
                outer = pltpu.roll(edge, 124 - 4 * (3 * x + n), 1)
                wm2 = jnp.where(lane < 2, outer, pltpu.roll(w, 2, 1))
                wp2 = jnp.where(lane >= 126, outer, pltpu.roll(w, 126, 1))
                wm1 = jnp.where(first, pltpu.roll(outer, 127, 1), pltpu.roll(w, 1, 1))
                wp1 = jnp.where(final, pltpu.roll(outer, 1, 1), pltpu.roll(w, 127, 1))
                at = 48 + 2 * (3 * x + n)
                um1 = jnp.where(first, pltpu.roll(below, 128 - at, 1), pltpu.roll(u, 1, 1))
                up1 = jnp.where(final, pltpu.roll(above, 126 - at, 1), pltpu.roll(u, 127, 1))
                own, low, high = side_terms(SPEED_Y, wm2, wm1, w, wp1, wp2, um1, u, up1)
                total = add_powers(total, [(low, um1), (high, up1), (own, u)])
            for k in range(6):
                out[k, x, z, :] = total[k]
        return carry

    lax.fori_loop(0, 64 // LONG, rows, 0)


def moments_of(nodes):
    total = [None] * 6
    for w, u in nodes:
        power = w
        for order in range(6):
            total[order] = power if total[order] is None else total[order] + power
            if order < 5:
                power = power * u
    return total


def invert(mom):
    inv0 = 1.0 / mom[0]
    a0 = mom[1] * inv0
    s1 = [None] + [mom[l + 1] - a0 * mom[l] for l in range(1, 5)]
    inv1 = 1.0 / s1[1]
    quot = s1[2] * inv1
    a1 = quot - a0
    b1 = s1[1] * inv0
    s2_two = s1[3] - a1 * s1[2] - b1 * mom[2]
    s2_three = s1[4] - a1 * s1[3] - b1 * mom[3]
    a2 = s2_three / s2_two - quot
    b2 = s2_two * inv1
    q = (a0 + a1 + a2) * (1.0 / 3.0)
    d0, d1, d2 = a0 - q, a1 - q, a2 - q
    square = (d0 * d0 + d1 * d1 + d2 * d2 + 2.0 * b1 + 2.0 * b2) * (1.0 / 6.0)
    p = jnp.sqrt(square)
    det = d0 * d1 * d2 - d0 * b2 - d2 * b1
    ratio = det / (2.0 * square * p)
    high = q + 2.0 * p * cos_third(ratio)
    low = q - 2.0 * p * cos_third(-ratio)
    middle = 3.0 * q - high - low
    both = b1 * b2
    scale = mom[0] * both
    nodes = []
    for value in (low, middle, high):
        e0 = value - a0
        e1 = (value - a1) * e0 - b1
        nodes.append((scale / (both + b2 * (e0 * e0) + e1 * e1), value))
    return nodes


def lanes(rows=ROWS):
    return lax.broadcasted_iota(jnp.int32, (rows, 128), 1)


def step_of(received):
    top = jnp.max(received[...], axis=0, keepdims=True)
    return COURANT / (SPEED_TOTAL * top)


def relay_kernel(own, got, mx):
    most = jnp.maximum(own[...], got[72:80, :])
    for i in range(mx.shape[0] // ROWS):
        mx[i * ROWS:(i + 1) * ROWS, :] = most


def entry_kernel(w, u, a, b, inner, zs, mx, sems):
    nodes = Nodes(a, b, inner)
    odd = odd_along("gx")
    loads = [
        pltpu.make_async_copy(array.at[n, plane_at(x, odd)], side(n, x), sems.at[at, n, x])
        for at, (array, side) in enumerate(((u, nodes.u), (w, nodes.w)))
        for n in range(3) for x in range(4)
    ]
    for copy in loads:
        copy.start()
    top = jnp.zeros((ROWS, 128), jnp.float32)
    for at in range(12):
        loads[at].wait()
        for i in range(64 // ROWS):
            top = jnp.maximum(top, jnp.abs(nodes.u(at // 4, at % 4)[i * ROWS:(i + 1) * ROWS, :]))
    for copy in loads[12:]:
        copy.wait()
    write_rows(nodes, top, zs, mx)


def edge_kernel(a, b, inner, ys):
    nodes, lane = Nodes(a, b, inner), lanes(EDGE)

    def rows(i, carry):
        z = rows_of(i, EDGE)
        packed = jnp.zeros((EDGE, 128), jnp.float32)
        for x in range(4):
            for n in range(3):
                at = 3 * x + n
                packed = jnp.where(lane // 4 == at, pltpu.roll(nodes.w(n, x)[z, :], 4 * at + 2, 1), packed)
                packed = jnp.where(lane // 2 == 24 + at, pltpu.roll(nodes.u(n, x)[z, :], 49 + 2 * at, 1), packed)
        ys[z, :] = packed
        return carry

    lax.fori_loop(0, 64 // EDGE, rows, 0)


def middle_kernel(change, a, b, inner, got, base, mid_a, mid_b, mid_inner, zs, mx):
    step = step_of(got)
    old, new = Nodes(a, b, inner), Nodes(mid_a, mid_b, mid_inner)

    def rows(i, top):
        z = rows_of(i)
        for x in range(4):
            mid = []
            for k, moment in enumerate(moments_of([(old.w(n, x)[z, :], old.u(n, x)[z, :]) for n in range(3)])):
                mid.append(moment - step * change[k, x, z, :])
                base[k, x, z, :] = 0.5 * (moment + mid[k])
            for n, (weight, speed) in enumerate(invert(mid)):
                new.w(n, x)[z, :] = weight
                new.u(n, x)[z, :] = speed
                top = jnp.maximum(top, jnp.abs(speed))
        return top

    top = lax.fori_loop(0, 64 // ROWS, rows, jnp.zeros((ROWS, 128), jnp.float32))
    write_rows(new, top, zs, mx)


def exit_kernel(change, base, got, out, held, sems):
    half = 0.5 * step_of(got)
    odd = odd_along("gx")
    stores = []
    for k in range(6):
        for x in range(4):
            held[k, x] = base[k, x] - half * change[k, x]
            stores.append(pltpu.make_async_copy(held.at[k, x], out.at[k, plane_at(x, odd)], sems.at[k, x]))
            stores[-1].start()
    for copy in stores:
        copy.wait()


def f32(*shape):
    return jax.ShapeDtypeStruct(shape, jnp.float32)


PLANES = (f32(9, 64, 128), f32(9, 64, 128), f32(6, 64, 128))
ROWS_Z, TOP = f32(80, 128), f32(ROWS, 128)
MOMENTS = f32(6, 4, 64, 128)
PADDED = [pltpu.VMEM((3, 4, 80, 128), jnp.float32)] * 2
VM = pl.BlockSpec(memory_space=pltpu.VMEM)
ANY = pl.BlockSpec(memory_space=pltpu.HBM)


def call(kernel, outs, args, scratch=(), ins=VM, out=VM, flops=1, limit=8 * 1024 * 1024):
    return pl.pallas_call(
        kernel,
        out_shape=outs,
        in_specs=[ins] * len(args),
        out_specs=out if isinstance(out, tuple) else jax.tree.map(lambda _: out, outs),
        scratch_shapes=list(scratch),
        cost_estimate=pl.CostEstimate(flops=flops, bytes_accessed=1 << 20, transcendentals=0),
        compiler_params=pltpu.CompilerParams(vmem_limit_bytes=limit),
    )(*args)


def pairs(n, first):
    return [(i, (i + 1) % n) for i in range(first, n, 2)] + [((i + 1) % n, i) for i in range(first, n, 2)]


def local(weights, abscissas):
    nx, ny, nz = (lax.axis_size(a) for a in ("gx", "gy", "gz"))
    swap = [(i, (i + 1) % nz) for i in range(nz)]

    def exchange(a, b, inner, zs, top):
        ys = call(edge_kernel, f32(64, 128), (a, b, inner), flops=1 << 20)
        halo = (
            lax.ppermute(a, "gx", pairs(nx, 0)),
            lax.ppermute(b, "gx", pairs(nx, 1)),
            lax.ppermute(zs, "gz", swap),
            lax.ppermute(ys, "gy", pairs(ny, 0)),
            lax.ppermute(ys, "gy", pairs(ny, 1)),
        )
        n = nx * ny
        top = call(relay_kernel, f32(n, 128), (top, halo[2]))
        got = lax.all_to_all(top.reshape(n, 1, 128), ("gx", "gy"), 0, 0)
        return halo, got.reshape(n, 128)

    def change_of(planes, xa, xb, zr, ya, yb):
        change = call(cross_kernel, MOMENTS, (*planes, xa, xb, zr), PADDED, flops=4 << 20)
        return call(along_kernel, MOMENTS, (change, *planes, ya, yb), flops=2 << 20)

    *planes, zs, top = call(
        entry_kernel, PLANES + (ROWS_Z, TOP), (weights, abscissas),
        [pltpu.SemaphoreType.DMA((2, 3, 4))], ins=ANY, limit=ENTRY_LIMIT)
    halo, got = exchange(*planes, zs, top)
    change = change_of(planes, *halo)
    base, *planes, zs, top = call(
        middle_kernel, (MOMENTS,) + PLANES + (ROWS_Z, TOP), (change, *planes, got), flops=4 << 20)
    halo, got = exchange(*planes, zs, top)
    change = change_of(planes, *halo)
    return call(
        exit_kernel, MOMENTS, (change, base, got),
        [pltpu.VMEM((6, 4, 64, 128), jnp.float32), pltpu.SemaphoreType.DMA((6, 4))], out=ANY)


def solution(mesh):
    spec = P(None, "gx", "gz", "gy")
    return jax.shard_map(local, mesh=mesh, in_specs=(spec, spec), out_specs=spec, check_vma=False)
```
